32 devices in a mesh: shard: 16 (over z, y, core), model: 2 (over x).
Axes of the slice: x: 2, y: 2, z: 4, core: 2. Of those that a mesh axis runs over, the one named last changes fastest.
Arguments:
- gradients: float32 [128, 128, 4096], P(None, 'shard', 'model'), may hold values from -6 to 6
- momentum: float32 [128, 128, 4096], P(None, 'shard', 'model'), may hold values from -6 to 6
- weights: float32 [128, 128, 4096], P(None, 'shard', 'model'), may hold values from -0.1875 to 0.1875
Outputs:
- new_weights: float32 [128, 128, 4096], P(None, 'shard', 'model')
- new_momentum: float32 [128, 128, 4096], P(None, 'shard', 'model')
The draws below stay inside these ranges and needn't reach their ends.
All inputs are finite; a program needn't handle non-finite values.
Results may differ from the reference program's by a relative error of at most 0.0001.
Values sent between devices are 32-bit elements; how exact they have to be, the bound alone decides.
A program may use at most 128 MiB of HBM per device.

```python
import jax
import jax.numpy as jnp
from jax import lax

SIDE = 128
WIDE = 4096
MATS = 128
ITERS = 3


def steps_of(stream_key, shape, pieces, low, largest):
    loudness, own = 1.0, jax.random.fold_in(stream_key, 6)
    for dim, parts in pieces:
        steps = jnp.exp(jax.random.uniform(jax.random.fold_in(own, dim), (parts,), jnp.float32, low / len(pieces), largest / len(pieces)))
        loudness = loudness * jnp.repeat(steps, shape[dim] // parts).reshape([-1 if axis == dim else 1 for axis in range(len(shape))])
    return loudness


def scatter_about(rng, shape, spread, bound, split=(), kind=jnp.bfloat16):
    entries = spread * jax.random.normal(rng, shape, jnp.float32)
    if split:
        entries = entries * steps_of(rng, shape, split, -0.22, 0.18)
    return jnp.clip(entries, -bound, bound).astype(kind)


def setup_inputs(seed: int = 0) -> dict:
    key_of = jax.random.split(jax.random.key(seed), 4)
    gradients = scatter_about(key_of[0], (MATS, SIDE, WIDE), 1.0, 6.0, ((1, 16), (2, 2)), jnp.float32)
    momentum = scatter_about(key_of[1], (MATS, SIDE, WIDE), 1.0, 6.0, ((1, 16), (2, 2)), jnp.float32)
    weights = scatter_about(key_of[2], (MATS, SIDE, WIDE), 0.03, 0.1875, ((1, 16), (2, 2)), jnp.float32)
    return dict(gradients=gradients, momentum=momentum, weights=weights)


hold_rate = 0.9
learn_rate = 0.9
decay_rate = 0.1

def reference(gradients, momentum, weights):
    new_momentum = hold_rate * momentum + gradients

    def orthogonal_one(stack):
        iterate = stack[None]
        iterate = iterate * lax.rsqrt(lax.optimization_barrier(jnp.sum(iterate * iterate, axis=(1, 2), keepdims=True)) + 1e-06)
        for step in range(ITERS):
            gram = jnp.einsum('mik,mjk->mij', iterate, iterate, precision=lax.Precision.HIGHEST)
            mixed = -4.775 * gram + 2.0315 * jnp.einsum('mij,mjk->mik', gram, gram, precision=lax.Precision.HIGHEST)
            iterate = 3.4445 * iterate + jnp.einsum('mij,mjk->mik', mixed, iterate, precision=lax.Precision.HIGHEST)
        return iterate[0]
    iterate = lax.map(orthogonal_one, new_momentum)
    new_weights = (1.0 - learn_rate * decay_rate) * weights - learn_rate * iterate
    return (new_weights, new_momentum)
```

```python
import functools

import jax
import jax.numpy as jnp
from jax import lax
from jax.experimental import pallas as pl
from jax.experimental.pallas import tpu as pltpu
from jax.sharding import PartitionSpec as P

ITERS = 3
AHEAD = 2

hold_rate = 0.9
learn_rate = 0.9
decay_rate = 0.1

MESH = pl.DeviceIdType.MESH


def dot(a, b, contract):
    return lax.dot_general(
        a,
        b,
        ((contract[0], contract[1]), ((), ())),
        precision=lax.Precision.HIGHEST,
        preferred_element_type=jnp.float32,
    )


def mul(a, b):
    return dot(a, b, ((1,), (0,)))


def mixer(gram, eye):
    total = jnp.sum(jnp.sum(gram * eye, axis=1, keepdims=True), axis=0, keepdims=True)
    scale = lax.rsqrt(total + 1e-06)
    a = gram * scale * scale
    q = None
    for step in range(ITERS):
        p = 3.4445 * eye + (-4.775 * a + 2.0315 * mul(a, a))
        q = p if q is None else mul(p, q)
        if step < ITERS - 1:
            a = mul(mul(p, a), p)
    return q * scale


def flipped(me, k, n):
    out, bit = 0, 1
    while bit < n:
        own = (me // bit) % 2
        out = out + bit * ((1 - own) if (k // bit) % 2 else own)
        bit *= 2
    return out


def exchange_kernel(n, models, moved_ref, back_ref, x, y, gram, peers, send1, recv1, send2, recv2, gsend, grecv):
    me = lax.axis_index("shard")
    col = lax.axis_index("model")
    mats, rows, cols = moved_ref.shape
    per = mats // n
    side = n * rows
    chunk = min(cols, 512)
    order = sorted(range(1, n), reverse=True)
    dests = [flipped(me, k, n) for k in order]
    mine = pl.ds(pl.multiple_of(me * rows, rows), rows)

    barrier = pltpu.get_barrier_semaphore()
    for dest in dests:
        pl.semaphore_signal(barrier, inc=1, device_id={"shard": dest}, device_id_type=MESH)
    for step in range(1, models):
        pl.semaphore_signal(barrier, inc=1, device_id={"model": (col + step) % models}, device_id_type=MESH)
    pl.semaphore_wait(barrier, n - 1 + models - 1)

    def forth(c):
        for dest in dests:
            pltpu.make_async_remote_copy(
                src_ref=moved_ref.at[dest * per + c],
                dst_ref=x.at[c, mine, :],
                send_sem=send1.at[c],
                recv_sem=recv1.at[c],
                device_id={"shard": dest},
                device_id_type=MESH,
            ).start()
        pltpu.make_async_copy(moved_ref.at[me * per + c], x.at[c, mine, :], recv1.at[c]).start()

    def back(c):
        for dest in dests:
            theirs = pl.ds(pl.multiple_of(dest * rows, rows), rows)
            pltpu.make_async_remote_copy(
                src_ref=y.at[c, theirs, :],
                dst_ref=back_ref.at[me * per + c],
                send_sem=send2.at[c],
                recv_sem=recv2,
                device_id={"shard": dest},
                device_id_type=MESH,
            ).start()
        pltpu.make_async_copy(y.at[c, mine, :], back_ref.at[me * per + c], recv2).start()

    for c in range(min(AHEAD, per)):
        forth(c)

    eye = (
        lax.broadcasted_iota(jnp.int32, (side, side), 0) == lax.broadcasted_iota(jnp.int32, (side, side), 1)
    ).astype(jnp.float32)

    def round_(c, carry):
        pltpu.make_async_copy(x.at[c], x.at[c], recv1.at[c]).wait()

        def part(k, total):
            piece = x[c, :, pl.ds(pl.multiple_of(k * chunk, chunk), chunk)]
            return total + dot(piece, piece, ((1,), (1,)))

        gram[c] = lax.fori_loop(0, cols // chunk, part, jnp.zeros((side, side), jnp.float32))

        @pl.when(c + AHEAD < per)
        def _():
            forth(c + AHEAD)

        copies = []
        for step in range(1, models):
            copy = pltpu.make_async_remote_copy(
                src_ref=gram.at[c],
                dst_ref=peers.at[step - 1, c],
                send_sem=gsend.at[step - 1, c],
                recv_sem=grecv.at[step - 1, c],
                device_id={"model": (col + step) % models},
                device_id_type=MESH,
            )
            copy.start()
            copies.append(copy)
        whole = gram[c]
        for step, copy in enumerate(copies):
            copy.wait()
            whole = whole + peers[step, c]
        q = mixer(whole, eye)

        def apply(k, carry):
            at = pl.ds(pl.multiple_of(k * chunk, chunk), chunk)
            y[c, :, at] = mul(q, x[c, :, at])
            return carry

        lax.fori_loop(0, cols // chunk, apply, 0)
        back(c)
        return carry

    lax.fori_loop(0, per, round_, 0)

    def drain(c, carry):
        sent = x.at[c, pl.ds(0, side - rows), :]
        pltpu.make_async_copy(sent, sent, send1.at[c]).wait()
        pltpu.make_async_copy(sent, sent, send2.at[c]).wait()
        return carry

    lax.fori_loop(0, per, drain, 0)
    pltpu.make_async_copy(back_ref, back_ref, recv2).wait()


def exchange(moved, n, models):
    mats, rows, cols = moved.shape
    per, side = mats // n, n * rows
    others = max(models - 1, 1)
    return pl.pallas_call(
        functools.partial(exchange_kernel, n, models),
        out_shape=jax.ShapeDtypeStruct(moved.shape, jnp.float32),
        in_specs=[pl.BlockSpec(memory_space=pl.ANY)],
        out_specs=pl.BlockSpec(memory_space=pl.ANY),
        scratch_shapes=[
            pltpu.VMEM((per, side, cols), jnp.float32),
            pltpu.VMEM((per, side, cols), jnp.float32),
            pltpu.VMEM((per, side, side), jnp.float32),
            pltpu.VMEM((others, per, side, side), jnp.float32),
            pltpu.SemaphoreType.DMA((per,)),
            pltpu.SemaphoreType.DMA((per,)),
            pltpu.SemaphoreType.DMA((per,)),
            pltpu.SemaphoreType.DMA,
            pltpu.SemaphoreType.DMA((others, per)),
            pltpu.SemaphoreType.DMA((others, per)),
        ],
        compiler_params=pltpu.CompilerParams(
            collective_id=0, has_side_effects=True, vmem_limit_bytes=48 * 1024 * 1024
        ),
    )(moved)


def exchange_plain(new_momentum):
    moved = lax.all_to_all(new_momentum, "shard", split_axis=0, concat_axis=1, tiled=True)
    gram = lax.psum(
        jnp.einsum("mik,mjk->mij", moved, moved, precision=lax.Precision.HIGHEST), "model"
    )
    eye = jnp.eye(gram.shape[-1], dtype=jnp.float32)
    q = jax.vmap(lambda g: mixer(g, eye))(gram)
    iterate = jnp.einsum("mij,mjk->mik", q, moved, precision=lax.Precision.HIGHEST)
    return lax.all_to_all(iterate, "shard", split_axis=1, concat_axis=0, tiled=True)


def body(n, models, gradients, momentum, weights):
    new_momentum = hold_rate * momentum + gradients
    mats, rows, cols = new_momentum.shape
    direct = n & (n - 1) == 0 and rows % 8 == 0 and cols % 128 == 0 and 2 * mats * rows * cols * 4 <= 32 << 20
    if direct:
        back = exchange(new_momentum, n, models)
    else:
        back = exchange_plain(new_momentum)
    new_weights = (1.0 - learn_rate * decay_rate) * weights - learn_rate * back
    return (new_weights, new_momentum)


def solution(mesh):
    placed = (P(None, "shard", "model"), P(None, "shard", "model"), P(None, "shard", "model"))
    return jax.shard_map(
        functools.partial(body, mesh.shape["shard"], mesh.shape["model"]),
        mesh=mesh,
        in_specs=placed,
        out_specs=(P(None, "shard", "model"), P(None, "shard", "model")),
        check_vma=False,
    )
```

```python
import functools

import jax
import jax.numpy as jnp
from jax import lax
from jax.experimental import pallas as pl
from jax.experimental.pallas import tpu as pltpu
from jax.sharding import PartitionSpec as P

ITERS = 3
AHEAD = 2
BEHIND = 3

hold_rate = 0.9
learn_rate = 0.9
decay_rate = 0.1

MESH = pl.DeviceIdType.MESH


def dot(a, b, contract):
    return lax.dot_general(
        a,
        b,
        ((contract[0], contract[1]), ((), ())),
        precision=lax.Precision.HIGHEST,
        preferred_element_type=jnp.float32,
    )


def mul(a, b):
    return dot(a, b, ((1,), (0,)))


def mixer(gram, eye):
    total = jnp.sum(jnp.sum(gram * eye, axis=1, keepdims=True), axis=0, keepdims=True)
    scale = lax.rsqrt(total + 1e-06)
    a = gram * scale * scale
    q = None
    for step in range(ITERS):
        p = 3.4445 * eye + (-4.775 * a + 2.0315 * mul(a, a))
        q = p if q is None else mul(p, q)
        if step < ITERS - 1:
            a = mul(mul(p, a), p)
    return q * scale


def flipped(me, k, n):
    out, bit = 0, 1
    while bit < n:
        own = (me // bit) % 2
        out = out + bit * ((1 - own) if (k // bit) % 2 else own)
        bit *= 2
    return out


def step_kernel(
    n, models, grad_ref, mom_ref, weight_ref, out_ref, new_ref,
    x, gs, ms, ws, gram, peers, gload, mload, wload, send1, recv1, send2, recv2, gsend, grecv,
):
    me = lax.axis_index("shard")
    col = lax.axis_index("model")
    _, per, rows, cols = grad_ref.shape
    side = n * rows
    chunk = min(cols, 512)
    dests = [flipped(me, k, n) for k in range(1, n)]
    mine = pl.ds(pl.multiple_of(me * rows, rows), rows)

    def loads(c):
        slot = c % 2
        return (
            pltpu.make_async_copy(grad_ref.at[:, c], gs.at[slot], gload.at[slot]),
            pltpu.make_async_copy(mom_ref.at[:, c], ms.at[slot], mload.at[slot]),
        )

    def weight_load(c):
        slot = c % 2
        return pltpu.make_async_copy(weight_ref.at[:, c], ws.at[slot], wload.at[slot])

    def load(c):
        for copy in loads(c):
            copy.start()

    def make(c):
        for copy in loads(c):
            copy.wait()
        slot = c % 2

        def one(j, carry):
            new_ref[j, c] = hold_rate * ms[slot, j] + gs[slot, j]
            return carry

        lax.fori_loop(0, n, one, 0)

    def finish(c):
        got = out_ref.at[:, c]
        pltpu.make_async_copy(got, got, recv2.at[c]).wait()
        weight_load(c).wait()
        slot = c % 2

        def one(j, carry):
            out_ref[j, c] = (1.0 - learn_rate * decay_rate) * ws[slot, j] - learn_rate * out_ref[j, c]
            return carry

        lax.fori_loop(0, n, one, 0)

    def forth(c):
        for dest in dests:
            pltpu.make_async_remote_copy(
                src_ref=new_ref.at[dest, c],
                dst_ref=x.at[c, mine, :],
                send_sem=send1.at[c],
                recv_sem=recv1.at[c],
                device_id={"shard": dest},
                device_id_type=MESH,
            ).start()
        pltpu.make_async_copy(new_ref.at[me, c], x.at[c, mine, :], recv1.at[c]).start()

    def back(c):
        for dest in dests:
            theirs = pl.ds(pl.multiple_of(dest * rows, rows), rows)
            pltpu.make_async_remote_copy(
                src_ref=x.at[c, theirs, :],
                dst_ref=out_ref.at[me, c],
                send_sem=send2.at[c],
                recv_sem=recv2.at[c],
                device_id={"shard": dest},
                device_id_type=MESH,
            ).start()
        pltpu.make_async_copy(x.at[c, mine, :], out_ref.at[me, c], recv2.at[c]).start()

    barrier = pltpu.get_barrier_semaphore()
    for dest in dests:
        pl.semaphore_signal(barrier, inc=1, device_id={"shard": dest}, device_id_type=MESH)
    for step in range(1, models):
        pl.semaphore_signal(barrier, inc=1, device_id={"model": (col + step) % models}, device_id_type=MESH)
    for c in range(min(2, per)):
        load(c)
        weight_load(c).start()
    make(0)
    pl.semaphore_wait(barrier, n - 1 + models - 1)
    forth(0)
    for c in range(2, min(AHEAD + 2, per + 1)):
        if c < per:
            load(c)
        make(c - 1)
    for c in range(1, min(AHEAD, per)):
        forth(c)

    eye = (
        lax.broadcasted_iota(jnp.int32, (side, side), 0) == lax.broadcasted_iota(jnp.int32, (side, side), 1)
    ).astype(jnp.float32)

    def round_(c, carry):
        pltpu.make_async_copy(x.at[c], x.at[c], recv1.at[c]).wait()

        def part(k, total):
            piece = x[c, :, pl.ds(pl.multiple_of(k * chunk, chunk), chunk)]
            return total + dot(piece, piece, ((1,), (1,)))

        gram[c] = lax.fori_loop(0, cols // chunk, part, jnp.zeros((side, side), jnp.float32))

        @pl.when(c + AHEAD < per)
        def _():
            forth(c + AHEAD)

        copies = []
        for step in range(1, models):
            copy = pltpu.make_async_remote_copy(
                src_ref=gram.at[c],
                dst_ref=peers.at[step - 1, c],
                send_sem=gsend.at[step - 1, c],
                recv_sem=grecv.at[step - 1, c],
                device_id={"model": (col + step) % models},
                device_id_type=MESH,
            )
            copy.start()
            copies.append(copy)
        whole = gram[c]
        for step, copy in enumerate(copies):
            copy.wait()
            whole = whole + peers[step, c]
        q = mixer(whole, eye)

        def apply(k, carry):
            at = pl.ds(pl.multiple_of(k * chunk, chunk), chunk)
            x[c, :, at] = mul(q, x[c, :, at])
            return carry

        lax.fori_loop(0, cols // chunk, apply, 0)

        @pl.when(c + AHEAD + 1 < per)
        def _():
            make(c + AHEAD + 1)

        @pl.when(c + AHEAD + 2 < per)
        def _():
            load(c + AHEAD + 2)

        back(c)

        @pl.when(c >= BEHIND)
        def _():
            finish(c - BEHIND)

            @pl.when(c - BEHIND + 2 < per)
            def _():
                weight_load(c - BEHIND + 2).start()

        return carry

    lax.fori_loop(0, per, round_, 0)

    def drain(c, carry):
        sent = x.at[c, pl.ds(0, side - rows), :]
        pltpu.make_async_copy(sent, sent, send1.at[c]).wait()
        return carry

    lax.fori_loop(0, per, drain, 0)

    def last(c, carry):
        finish(c)

        @pl.when(c + 2 < per)
        def _():
            weight_load(c + 2).start()

        return carry

    lax.fori_loop(max(per - BEHIND, 0), per, last, 0)

    def drain_back(c, carry):
        sent = x.at[c, pl.ds(0, side - rows), :]
        pltpu.make_async_copy(sent, sent, send2.at[c]).wait()
        return carry

    lax.fori_loop(0, per, drain_back, 0)


def step_direct(gradients, momentum, weights, n, models):
    mats, rows, cols = gradients.shape
    per, side = mats // n, n * rows
    others = max(models - 1, 1)
    split = (n, per, rows, cols)
    placed = pltpu.VMEM(split, jnp.float32)
    out, new = pl.pallas_call(
        functools.partial(step_kernel, n, models),
        out_shape=(placed, placed),
        in_specs=[pl.BlockSpec(memory_space=pltpu.HBM)] * 3,
        out_specs=[pl.BlockSpec(memory_space=pltpu.VMEM)] * 2,
        scratch_shapes=[
            pltpu.VMEM((per, side, cols), jnp.float32),
            pltpu.VMEM((2, n, rows, cols), jnp.float32),
            pltpu.VMEM((2, n, rows, cols), jnp.float32),
            pltpu.VMEM((2, n, rows, cols), jnp.float32),
            pltpu.VMEM((per, side, side), jnp.float32),
            pltpu.VMEM((others, per, side, side), jnp.float32),
            pltpu.SemaphoreType.DMA((2,)),
            pltpu.SemaphoreType.DMA((2,)),
            pltpu.SemaphoreType.DMA((2,)),
            pltpu.SemaphoreType.DMA((per,)),
            pltpu.SemaphoreType.DMA((per,)),
            pltpu.SemaphoreType.DMA((per,)),
            pltpu.SemaphoreType.DMA((per,)),
            pltpu.SemaphoreType.DMA((others, per)),
            pltpu.SemaphoreType.DMA((others, per)),
        ],
        compiler_params=pltpu.CompilerParams(
            collective_id=0, has_side_effects=True, vmem_limit_bytes=40 * 1024 * 1024
        ),
    )(*(array.reshape(split) for array in (gradients, momentum, weights)))
    return out.reshape(gradients.shape), new.reshape(gradients.shape)


def exchange_plain(new_momentum):
    moved = lax.all_to_all(new_momentum, "shard", split_axis=0, concat_axis=1, tiled=True)
    gram = lax.psum(
        jnp.einsum("mik,mjk->mij", moved, moved, precision=lax.Precision.HIGHEST), "model"
    )
    eye = jnp.eye(gram.shape[-1], dtype=jnp.float32)
    q = jax.vmap(lambda g: mixer(g, eye))(gram)
    iterate = jnp.einsum("mij,mjk->mik", q, moved, precision=lax.Precision.HIGHEST)
    return lax.all_to_all(iterate, "shard", split_axis=1, concat_axis=0, tiled=True)


def body(n, models, gradients, momentum, weights):
    mats, rows, cols = gradients.shape
    size = mats * rows * cols * 4
    if n & (n - 1) == 0 and rows % 8 == 0 and cols % 128 == 0 and size <= 8 << 20 and mats // n > BEHIND:
        return step_direct(gradients, momentum, weights, n, models)
    new_momentum = hold_rate * momentum + gradients
    back = exchange_plain(new_momentum)
    new_weights = (1.0 - learn_rate * decay_rate) * weights - learn_rate * back
    return (new_weights, new_momentum)


def solution(mesh):
    placed = (P(None, "shard", "model"), P(None, "shard", "model"), P(None, "shard", "model"))
    return jax.shard_map(
        functools.partial(body, mesh.shape["shard"], mesh.shape["model"]),
        mesh=mesh,
        in_specs=placed,
        out_specs=(P(None, "shard", "model"), P(None, "shard", "model")),
        check_vma=False,
    )
```
